32 devices in a mesh: blk: 8 (over y, x, core), layer: 4 (over z).
Axes of the slice: x: 2, y: 2, z: 4, core: 2. Of those that a mesh axis runs over, the one named last changes fastest.
Arguments:
- points: float32 [8192, 128], P('blk'), may hold values from -6 to 6
- inv_scale: float32 [128], replicated, may hold values from 0.01 to 0.25
- vectors: float32 [8192, 64], P('blk'), may hold values from -6 to 6
- noise: float32 [8192], P(('blk', 'layer')), may hold values from 0.1 to 1
Outputs:
- result: float32 [8192, 64], P(('blk', 'layer'))
The draws below stay inside these ranges and needn't reach their ends.
All inputs are finite; a program needn't handle non-finite values.
Results may differ from the reference program's by a relative error of at most 0.0001.
Values sent between devices are 32-bit elements; how exact they have to be, the bound alone decides.
A program may use at most 64 MiB of HBM per device.

```python
import math
import jax
import jax.numpy as jnp
from jax import lax

FEATS = 128
RHS = 64
BLOCK = 1024
NPTS = 8192
N_BLK = 8
N_LAYER = 4


def shard_levels(stream_key, dims, pieces, low, top_value):
    gain, own = 1.0, jax.random.fold_in(stream_key, 6)
    for axis_at, blocks in pieces:
        draws = jnp.exp(jax.random.uniform(jax.random.fold_in(own, axis_at), (blocks,), jnp.float32, low / len(pieces), top_value / len(pieces)))
        gain = gain * jnp.repeat(draws, dims[axis_at] // blocks).reshape([-1 if axis == axis_at else 1 for axis in range(len(dims))])
    return gain


def centred(own_key, extent, deviation, reach, pieces=(), held_as=jnp.bfloat16):
    gain = shard_levels(own_key, extent, pieces, -0.22, 0.18) if pieces else 1.0
    result = jax.random.normal(own_key, extent, jnp.float32) * deviation * gain
    return jnp.minimum(jnp.maximum(result, -reach), reach).astype(held_as)


def setup_inputs(seed: int = 0) -> dict:
    key_of = jax.random.split(jax.random.key(seed), 5)
    return {
        "points": centred(key_of[0], (NPTS, FEATS), 1.0, 6.0, ((0, 8),), jnp.float32),
        "inv_scale": jnp.clip(jnp.exp(jax.random.uniform(key_of[1], (FEATS,), jnp.float32, math.log(0.01), math.log(0.25))), 0.01, 0.25),
        "vectors": centred(key_of[2], (NPTS, RHS), 1.0, 6.0, ((0, 8),), jnp.float32),
        "noise": jnp.clip(jnp.exp(math.log(1.0) - 2.3025851 * jax.random.uniform(key_of[3], (NPTS,), jnp.float32) ** shard_levels(key_of[3], (NPTS,), ((0, 32),), -0.2, 0.2)), 0.1, 1.0),
    }


ROOT_FIVE = 5.0 ** 0.5
FIVE_THIRDS = 5.0 / 3.0

def matern(left_scaled, right_scaled):
    left_norms = lax.optimization_barrier(jnp.sum(left_scaled * left_scaled, axis=1))
    right_norms = lax.optimization_barrier(jnp.sum(right_scaled * right_scaled, axis=1))
    cross = jnp.dot(left_scaled, right_scaled.T, precision=lax.Precision.HIGHEST, preferred_element_type=jnp.float32)
    distance_sq = jnp.maximum(left_norms[:, None] + right_norms[None, :] - 2.0 * cross, 0.0)
    radius = jnp.sqrt(distance_sq)
    return (1.0 + ROOT_FIVE * radius + FIVE_THIRDS * distance_sq) * jnp.exp(-ROOT_FIVE * radius)

def tile_pair(members):
    left_scaled, right_scaled, left_vectors, right_vectors = members
    kernel = matern(left_scaled, right_scaled)
    direct = jnp.dot(kernel, right_vectors, precision=lax.Precision.HIGHEST, preferred_element_type=jnp.float32)
    mirrored = jnp.dot(kernel.T, left_vectors, precision=lax.Precision.HIGHEST, preferred_element_type=jnp.float32)
    return (direct, mirrored)

def reference(points, inv_scale, vectors, noise):
    scaled = (points * inv_scale[None, :]).reshape(N_BLK, BLOCK, FEATS)
    grouped = vectors.reshape(N_BLK, BLOCK, RHS)
    summed = jnp.zeros((N_BLK, BLOCK, RHS), jnp.float32)
    for distance in range(N_LAYER):
        partner_scaled = jnp.roll(scaled, -distance, axis=0)
        partner_vectors = jnp.roll(grouped, -distance, axis=0)
        direct, mirrored = lax.map(tile_pair, (scaled, partner_scaled, grouped, partner_vectors))
        summed = summed + direct
        if distance > 0:
            summed = summed + jnp.roll(mirrored, distance, axis=0)
    normalizer = float(BLOCK * (2 * N_LAYER - 1)) ** (-0.5)
    return summed.reshape(NPTS, RHS) * normalizer + noise[:, None] * vectors
```

```python
import functools
import math

import jax
import jax.numpy as jnp
from jax import lax
from jax.experimental import pallas as pl
from jax.experimental.pallas import tpu as pltpu
from jax.sharding import PartitionSpec as P

MESH = pl.DeviceIdType.MESH
LOG2 = math.log(2.0)
UNIT = math.sqrt(5.0) / LOG2
SHIFT = 1.5 / LOG2
REST = 3.0 / LOG2**2 - SHIFT**2
GAIN = LOG2**2 / 3.0 * 2.0**SHIFT
BF16 = jnp.bfloat16
F32 = jnp.float32


def two_terms(value):
    high = value.astype(BF16).astype(F32)
    return high, (value - high).astype(BF16).astype(F32)


def augmented(points, scale, left):
    high, low = two_terms(points * scale)
    held = high + low
    norm = jnp.sum(held * held, axis=1, keepdims=True)
    first = norm.astype(BF16).astype(F32)
    second = (norm - first).astype(BF16).astype(F32)
    third = norm - first - second
    lane = lax.broadcasted_iota(jnp.int32, high.shape, 1)
    at, ones = (0, 3) if left else (3, 0)
    extra = jnp.where(
        lane == at,
        first,
        jnp.where(
            lane == at + 1,
            second,
            jnp.where(
                lane == at + 2,
                third,
                jnp.where((lane >= ones) & (lane < ones + 3), 1.0, 0.0),
            ),
        ),
    )
    if left:
        high, low = -2.0 * high, -2.0 * low
        terms = (high, high, low, extra)
    else:
        terms = (high, low, high, extra)
    return jnp.concatenate([term.astype(BF16) for term in terms], axis=1)


def nt_dot(left, right):
    return lax.dot_general(left, right, (((1,), (1,)), ((), ())), preferred_element_type=F32)


def kernel(
    chips, layers, tile, points, scale, vectors, noise, out,
    p_data, v_data, s_data, n_data, q_in, left, v_left, right, high, low, r_out, r_in,
    own_sem, p_send, p_recv, v_send, v_recv, q_send, q_recv, r_send, r_recv,
):
    block, layer = lax.axis_index("blk"), lax.axis_index("layer")
    core = lax.rem(block, 2)
    chip = block // 2
    rows, columns = p_data.shape[1], v_data.shape[1]
    piece = rows // layers
    mine = pl.ds(pl.multiple_of(layer * piece, piece), piece)
    sibling = (block + 1 - 2 * core, layer)
    others = range(1, chips)

    def peer(i):
        return (2 * (chip ^ i) + core, layer)

    barrier = pltpu.get_barrier_semaphore()
    for target in (*(peer(i) for i in others), sibling):
        pl.semaphore_signal(barrier, inc=1, device_id=target, device_id_type=MESH)

    own = (
        pltpu.make_async_copy(points, p_data.at[0], own_sem.at[0]),
        pltpu.make_async_copy(scale, s_data, own_sem.at[1]),
        pltpu.make_async_copy(vectors, v_data.at[0], own_sem.at[2]),
        pltpu.make_async_copy(noise, n_data, own_sem.at[3]),
    )
    for copy in own:
        copy.start()

    def query(i):
        return pltpu.make_async_remote_copy(
            p_data.at[0, mine], q_in.at[i - 1], q_send.at[i - 1], q_recv.at[i - 1], peer(i), MESH
        )

    def result(i):
        return pltpu.make_async_remote_copy(
            r_out.at[i - 1], r_in.at[i - 1], r_send.at[i - 1], r_recv.at[i - 1], peer(i), MESH
        )

    across = (
        pltpu.make_async_remote_copy(p_data.at[0], p_data.at[1], p_send, p_recv, sibling, MESH),
        pltpu.make_async_remote_copy(v_data.at[0], v_data.at[1], v_send, v_recv, sibling, MESH),
    )

    for copy in own:
        copy.wait()
    pl.semaphore_wait(barrier, chips)
    for i in others:
        query(i).start()
    for copy in across:
        copy.start()

    unit = s_data[...] * UNIT

    def prepare(slot):
        left[slot] = augmented(p_data[slot], unit, True)
        v_left[slot] = jnp.concatenate(two_terms(v_data[slot]), axis=0).astype(BF16)

    def product(slot):
        for start in range(0, rows, tile):
            at = pl.ds(start, tile)
            square = jnp.maximum(nt_dot(left[slot, at, :], right[...]), 1e-20)
            z = -SHIFT - square * lax.rsqrt(square)
            value = (z * z + REST) * jnp.exp2(z)
            high[at, :] = value.astype(BF16)
            low[at, :] = (value - value.astype(BF16).astype(F32)).astype(BF16)
        turned = jnp.dot(v_left[slot], high[...], preferred_element_type=F32)
        turned_low = jnp.dot(v_left[slot, :columns], low[...], preferred_element_type=F32)
        return turned[:columns] + turned[columns:] + turned_low

    prepare(0)
    right[...] = augmented(p_data[0, mine], unit, False)
    total = product(0)
    for copy in across:
        copy.wait()
    prepare(1)
    total += product(1)

    for i in others:
        query(i).wait()
        right[...] = augmented(q_in[i - 1], unit, False)
        partial = product(1)
        if 2 * i != chips:
            partial += product(0)
        r_out[i - 1] = partial
        result(i).start()

    for i in others:
        result(i).wait()
        total += r_in[i - 1]
    normalizer = GAIN * float(rows * (2 * layers - 1)) ** (-0.5)
    held = v_data[0, :, pl.ds(pl.multiple_of(layer * piece, 128), piece)]
    out[...] = total * normalizer + n_data[...] * held


def per_device(points, inv_scale, vectors, noise):
    blocks, layers = lax.axis_size("blk"), lax.axis_size("layer")
    chips = blocks // 2
    rows, features = points.shape
    columns = vectors.shape[1]
    piece = rows // layers
    assert blocks == 2 * layers and chips & (chips - 1) == 0
    tile = min(256, rows)
    hbm = pl.BlockSpec(memory_space=pl.ANY)
    dma = pltpu.SemaphoreType.DMA
    peers = chips - 1
    out = pl.pallas_call(
        functools.partial(kernel, chips, layers, tile),
        out_shape=pltpu.VMEM((columns, piece), F32),
        in_specs=[hbm] * 4,
        out_specs=pl.BlockSpec(memory_space=pltpu.VMEM),
        scratch_shapes=[
            pltpu.VMEM((2, rows, features), F32),
            pltpu.VMEM((2, columns, rows), F32),
            pltpu.VMEM((1, features), F32),
            pltpu.VMEM((1, piece), F32),
            pltpu.VMEM((peers, piece, features), F32),
            pltpu.VMEM((2, rows, 4 * features), BF16),
            pltpu.VMEM((2, 2 * columns, rows), BF16),
            pltpu.VMEM((piece, 4 * features), BF16),
            pltpu.VMEM((rows, piece), BF16),
            pltpu.VMEM((rows, piece), BF16),
            pltpu.VMEM((peers, columns, piece), F32),
            pltpu.VMEM((peers, columns, piece), F32),
            dma((4,)),
            *[dma(()) for _ in range(4)],
            *[dma((peers,)) for _ in range(4)],
        ],
        compiler_params=pltpu.CompilerParams(collective_id=0, has_side_effects=True),
    )(points, inv_scale[None, :], vectors.T, noise[None, :])
    return out.T


def solution(mesh):
    placed = (P("blk", None), P(), P("blk", None), P(("blk", "layer")))
    return jax.shard_map(
        per_device, mesh=mesh, in_specs=placed, out_specs=P(("blk", "layer"), None), check_vma=False
    )
```

```python
import functools
import math

import jax
import jax.numpy as jnp
from jax import lax
from jax.experimental import pallas as pl
from jax.experimental.pallas import tpu as pltpu
from jax.sharding import PartitionSpec as P

MESH = pl.DeviceIdType.MESH
LOG2 = math.log(2.0)
UNIT = math.sqrt(5.0) / LOG2
SHIFT = 1.5 / LOG2
REST = 3.0 / LOG2**2 - SHIFT**2
GAIN = LOG2**2 / 3.0 * 2.0**SHIFT
BF16 = jnp.bfloat16
F32 = jnp.float32


def two_terms(value):
    high = value.astype(BF16).astype(F32)
    return high, (value - high).astype(BF16).astype(F32)


def augmented(points, scale, left):
    high, low = two_terms(points * scale)
    held = high + low
    norm = jnp.sum(held * held, axis=1, keepdims=True)
    first = norm.astype(BF16).astype(F32)
    second = (norm - first).astype(BF16).astype(F32)
    third = norm - first - second
    lane = lax.broadcasted_iota(jnp.int32, high.shape, 1)
    at, ones = (0, 3) if left else (3, 0)
    extra = jnp.where(
        lane == at,
        first,
        jnp.where(
            lane == at + 1,
            second,
            jnp.where(
                lane == at + 2,
                third,
                jnp.where((lane >= ones) & (lane < ones + 3), 1.0, 0.0),
            ),
        ),
    )
    if left:
        high, low = -2.0 * high, -2.0 * low
        terms = (high, high, low, extra)
    else:
        terms = (high, low, high, extra)
    return jnp.concatenate([term.astype(BF16) for term in terms], axis=1)


def nt_dot(left, right):
    return lax.dot_general(left, right, (((1,), (1,)), ((), ())), preferred_element_type=F32)


def kernel(
    chips, layers, tile, points, scale, vectors, noise, out,
    p_data, v_data, s_data, n_data, q_in, left, v_left, right, high, low, r_out, r_in,
    own_sem, p_send, p_recv, v_send, v_recv, q_send, q_recv, r_send, r_recv,
):
    block, layer = lax.axis_index("blk"), lax.axis_index("layer")
    core = lax.rem(block, 2)
    chip = block // 2
    rows, columns = p_data.shape[1], v_data.shape[1]
    piece = rows // layers
    mine = pl.ds(pl.multiple_of(layer * piece, piece), piece)
    sibling = (block + 1 - 2 * core, layer)
    others = range(1, chips)
    bits = [1 << d for d in range(chips.bit_length() - 1)]
    half = piece // 2

    def peer(i):
        return (2 * (chip ^ i) + core, layer)

    barrier = pltpu.get_barrier_semaphore()
    for target in (*(peer(bit) for bit in bits), sibling):
        pl.semaphore_signal(barrier, inc=1, device_id=target, device_id_type=MESH)

    own = (
        pltpu.make_async_copy(points, p_data.at[0], own_sem.at[0]),
        pltpu.make_async_copy(scale, s_data, own_sem.at[1]),
        pltpu.make_async_copy(vectors, v_data.at[0], own_sem.at[2]),
        pltpu.make_async_copy(noise, n_data, own_sem.at[3]),
    )
    for copy in own:
        copy.start()

    def last_bit(i, h):
        return i & -i if h else 1 << (i.bit_length() - 1)

    def nth(i, turn):
        return turn if i * i < chips else 1 - turn

    def query(i, h):
        bit = last_bit(i, h)
        before = i ^ bit
        at = pl.ds(pl.multiple_of(layer * piece + h * half, half), half)
        return pltpu.make_async_remote_copy(
            q_in.at[before - 1, h] if before else p_data.at[0, at],
            q_in.at[i - 1, h],
            q_send.at[i - 1, h],
            q_recv.at[i - 1, h],
            peer(bit),
            MESH,
        )

    def relay(i, h):
        for j in others:
            if j ^ last_bit(j, h) == i:
                query(j, h).start()

    def result(i):
        return pltpu.make_async_remote_copy(
            r_out.at[i - 1], r_in.at[i - 1], r_send.at[i - 1], r_recv.at[i - 1], peer(i), MESH
        )

    across = (
        pltpu.make_async_remote_copy(p_data.at[0], p_data.at[1], p_send, p_recv, sibling, MESH),
        pltpu.make_async_remote_copy(v_data.at[0], v_data.at[1], v_send, v_recv, sibling, MESH),
    )

    for copy in own:
        copy.wait()
    unit = s_data[...] * UNIT

    def prepare(slot):
        left[slot] = augmented(p_data[slot], unit, True)
        v_left[slot] = jnp.concatenate(two_terms(v_data[slot]), axis=0).astype(BF16)

    def product(slot):
        for start in range(0, rows, tile):
            at = pl.ds(start, tile)
            square = jnp.maximum(nt_dot(left[slot, at, :], right[...]), 1e-20)
            z = -SHIFT - square * lax.rsqrt(square)
            value = (z * z + REST) * jnp.exp2(z)
            high[at, :] = value.astype(BF16)
            low[at, :] = (value - value.astype(BF16).astype(F32)).astype(BF16)
        turned = jnp.dot(v_left[slot], high[...], preferred_element_type=F32)
        turned_low = jnp.dot(v_left[slot, :columns], low[...], preferred_element_type=F32)
        return turned[:columns] + turned[columns:] + turned_low

    prepare(0)
    right[...] = augmented(p_data[0, mine], unit, False)
    pl.semaphore_wait(barrier, 1 + len(bits))
    for turn in (0, 1):
        for bit in bits:
            query(bit, nth(bit, turn)).start()
    for copy in across:
        copy.start()
    total = product(0)
    for copy in across:
        copy.wait()
    prepare(1)
    total += product(1)

    for count in range(1, len(bits) + 1):
        level = [i for i in others if i.bit_count() == count]
        for i in level:
            query(i, nth(i, 0)).wait_recv()
            relay(i, nth(i, 0))
        for i in level:
            query(i, nth(i, 1)).wait_recv()
            relay(i, nth(i, 1))
            both = jnp.concatenate([q_in[i - 1, 0], q_in[i - 1, 1]], axis=0)
            right[...] = augmented(both, unit, False)
            partial = product(1)
            if 2 * i != chips:
                partial += product(0)
            r_out[i - 1] = partial
            result(i).start()

    for i in others:
        for h in (0, 1):
            query(i, h).wait_send()
        result(i).wait()
        total += r_in[i - 1]
    normalizer = GAIN * float(rows * (2 * layers - 1)) ** (-0.5)
    held = v_data[0, :, pl.ds(pl.multiple_of(layer * piece, 128), piece)]
    out[...] = total * normalizer + n_data[...] * held


def per_device(points, inv_scale, vectors, noise):
    blocks, layers = lax.axis_size("blk"), lax.axis_size("layer")
    chips = blocks // 2
    rows, features = points.shape
    columns = vectors.shape[1]
    piece = rows // layers
    assert blocks == 2 * layers and chips & (chips - 1) == 0
    tile = min(256, rows)
    hbm = pl.BlockSpec(memory_space=pl.ANY)
    dma = pltpu.SemaphoreType.DMA
    peers = chips - 1
    out = pl.pallas_call(
        functools.partial(kernel, chips, layers, tile),
        out_shape=pltpu.VMEM((columns, piece), F32),
        in_specs=[hbm] * 4,
        out_specs=pl.BlockSpec(memory_space=pltpu.VMEM),
        scratch_shapes=[
            pltpu.VMEM((2, rows, features), F32),
            pltpu.VMEM((2, columns, rows), F32),
            pltpu.VMEM((1, features), F32),
            pltpu.VMEM((1, piece), F32),
            pltpu.VMEM((peers, 2, piece // 2, features), F32),
            pltpu.VMEM((2, rows, 4 * features), BF16),
            pltpu.VMEM((2, 2 * columns, rows), BF16),
            pltpu.VMEM((piece, 4 * features), BF16),
            pltpu.VMEM((rows, piece), BF16),
            pltpu.VMEM((rows, piece), BF16),
            pltpu.VMEM((peers, columns, piece), F32),
            pltpu.VMEM((peers, columns, piece), F32),
            dma((4,)),
            *[dma(()) for _ in range(4)],
            *[dma((peers, 2)) for _ in range(2)],
            *[dma((peers,)) for _ in range(2)],
        ],
        compiler_params=pltpu.CompilerParams(collective_id=0, has_side_effects=True),
    )(points, inv_scale[None, :], vectors.T, noise[None, :])
    return out.T


def solution(mesh):
    placed = (P("blk", None), P(), P("blk", None), P(("blk", "layer")))
    return jax.shard_map(
        per_device, mesh=mesh, in_specs=placed, out_specs=P(("blk", "layer"), None), check_vma=False
    )
```

```python
import functools
import math

import jax
import jax.numpy as jnp
from jax import lax
from jax.experimental import pallas as pl
from jax.experimental.pallas import tpu as pltpu
from jax.sharding import PartitionSpec as P

MESH = pl.DeviceIdType.MESH
LOG2 = math.log(2.0)
UNIT = math.sqrt(5.0) / LOG2
SHIFT = 1.5 / LOG2
REST = 3.0 / LOG2**2 - SHIFT**2
GAIN = LOG2**2 / 3.0 * 2.0**SHIFT
BF16 = jnp.bfloat16
F32 = jnp.float32


def two_terms(value):
    high = value.astype(BF16).astype(F32)
    return high, (value - high).astype(BF16).astype(F32)


def augmented(points, scale, left):
    high, low = two_terms(points * scale)
    held = high + low
    norm = jnp.sum(held * held, axis=1, keepdims=True)
    first = norm.astype(BF16).astype(F32)
    second = (norm - first).astype(BF16).astype(F32)
    third = norm - first - second
    lane = lax.broadcasted_iota(jnp.int32, high.shape, 1)
    at, ones = (0, 3) if left else (3, 0)
    extra = jnp.where(
        lane == at,
        first,
        jnp.where(
            lane == at + 1,
            second,
            jnp.where(
                lane == at + 2,
                third,
                jnp.where((lane >= ones) & (lane < ones + 3), 1.0, 0.0),
            ),
        ),
    )
    if left:
        high, low = -2.0 * high, -2.0 * low
        terms = (high, high, low, extra)
    else:
        terms = (high, low, high, extra)
    return jnp.concatenate([term.astype(BF16) for term in terms], axis=1)


def nt_dot(left, right):
    return lax.dot_general(left, right, (((1,), (1,)), ((), ())), preferred_element_type=F32)


def kernel(
    chips, layers, parts, tile, points, scale, vectors, noise, out,
    p_data, v_data, s_data, n_data, q_in, left, v_left, right, high, low, r_out, r_in,
    own_sem, p_send, p_recv, v_send, v_recv, q_send, q_recv, r_send, r_recv,
):
    block, layer = lax.axis_index("blk"), lax.axis_index("layer")
    core = lax.rem(block, 2)
    chip = block // 2
    rows, columns = p_data.shape[1], v_data.shape[1]
    piece = rows // layers
    mine = pl.ds(pl.multiple_of(layer * piece, piece), piece)
    sibling = (block + 1 - 2 * core, layer)
    others = range(1, chips)
    bits = [1 << d for d in range(chips.bit_length() - 1)]
    part = piece // parts

    def peer(i, same=False):
        return (2 * (chip ^ i) + (core if same else 1 - core), layer)

    barrier = pltpu.get_barrier_semaphore()
    for target in (*(peer(bit, same) for bit in bits for same in (False, True)), sibling):
        pl.semaphore_signal(barrier, inc=1, device_id=target, device_id_type=MESH)

    own = (
        pltpu.make_async_copy(points, p_data.at[0], own_sem.at[0]),
        pltpu.make_async_copy(scale, s_data, own_sem.at[1]),
        pltpu.make_async_copy(vectors, v_data.at[0], own_sem.at[2]),
        pltpu.make_async_copy(noise, n_data, own_sem.at[3]),
    )
    for copy in own:
        copy.start()

    def last_bit(i, h):
        return i & -i if 2 * h >= parts else 1 << (i.bit_length() - 1)

    def nth(i, turn):
        return turn if i * i < chips else (turn + parts // 2) % parts

    def query(i, h):
        bit = last_bit(i, h)
        before = i ^ bit
        at = pl.ds(pl.multiple_of(layer * piece + h * part, part), part)
        return pltpu.make_async_remote_copy(
            q_in.at[before - 1, h] if before else p_data.at[0, at],
            q_in.at[i - 1, h],
            q_send.at[i - 1, h],
            q_recv.at[i - 1, h],
            peer(bit, same=before > 0),
            MESH,
        )

    def relay(i, h):
        for j in others:
            if j ^ last_bit(j, h) == i:
                query(j, h).start()

    def result(i):
        return pltpu.make_async_remote_copy(
            r_out.at[i - 1], r_in.at[i - 1], r_send.at[i - 1], r_recv.at[i - 1], peer(i), MESH
        )

    across = (
        pltpu.make_async_remote_copy(p_data.at[0], p_data.at[1], p_send, p_recv, sibling, MESH),
        pltpu.make_async_remote_copy(v_data.at[0], v_data.at[1], v_send, v_recv, sibling, MESH),
    )

    for copy in own:
        copy.wait()
    unit = s_data[...] * UNIT

    def prepare(slot):
        left[slot] = augmented(p_data[slot], unit, True)
        v_left[slot] = jnp.concatenate(two_terms(v_data[slot]), axis=0).astype(BF16)

    def evaluate(queries, slot, buffer):
        for start in range(0, rows, tile):
            at = pl.ds(start, tile)
            square = jnp.maximum(nt_dot(left[slot, at, :], queries), 1e-20)
            z = -SHIFT - square * lax.rsqrt(square)
            value = (z * z + REST) * jnp.exp2(z)
            high[buffer, at, :] = value.astype(BF16)
            low[buffer, at, :] = (value - value.astype(BF16).astype(F32)).astype(BF16)

    def product(slot, buffer):
        turned = jnp.dot(v_left[slot], high[buffer], preferred_element_type=F32)
        turned_low = jnp.dot(v_left[slot, :columns], low[buffer], preferred_element_type=F32)
        return turned[:columns] + turned[columns:] + turned_low

    def receive(i, h):
        query(i, h).wait_recv()
        relay(i, h)

    def expand(i, h):
        right[i, pl.ds(h * part, part)] = augmented(q_in[i - 1, h], unit, False)

    def answer(i, partial):
        r_out[i - 1] = partial
        result(i).start()

    pl.semaphore_wait(barrier, 1 + 2 * len(bits))
    for turn in range(parts):
        for bit in bits:
            query(bit, nth(bit, turn)).start()
    for copy in across:
        copy.start()
    prepare(0)
    right[0] = augmented(p_data[0, mine], unit, False)
    evaluate(right[0], 0, 0)
    for copy in across:
        copy.wait()
    prepare(1)
    evaluate(right[0], 1, 1)
    total = product(0, 0) + product(1, 1)

    near, far = 1, chips // 2
    half = piece // 2
    for turn in range(parts):
        for bit in bits:
            receive(bit, nth(bit, turn))
        if 2 * turn + 2 == parts:
            for bit in bits:
                for done in range(turn + 1):
                    expand(bit, nth(bit, done))
            mixed = jnp.concatenate([right[near, :half], right[far, half:]], axis=0)
            evaluate(mixed, 0, 0)
    for bit in bits:
        for turn in range(parts // 2, parts):
            expand(bit, nth(bit, turn))
    mixed = jnp.concatenate([right[near, half:], right[far, :half]], axis=0)
    evaluate(mixed, 0, 1)
    first = product(0, 0)
    evaluate(right[near], 1, 0)
    second = product(0, 1)
    answer(far, jnp.concatenate([second[:, half:], first[:, half:]], axis=1))
    crossed = jnp.concatenate([first[:, :half], second[:, :half]], axis=1)
    answer(near, crossed + product(1, 0))

    for count in range(1, len(bits) + 1):
        level = [i for i in others if i.bit_count() == count and i not in (near, far)]
        for i in level:
            if count > 1:
                for turn in range(parts):
                    receive(i, nth(i, turn))
                for h in range(parts):
                    expand(i, h)
            evaluate(right[i], 0, 0)
            evaluate(right[i], 1, 1)
            answer(i, product(0, 0) + product(1, 1))

    for i in others:
        for h in range(parts):
            query(i, h).wait_send()
        result(i).wait()
        total += r_in[i - 1]
    normalizer = GAIN * float(rows * (2 * layers - 1)) ** (-0.5)
    held = v_data[0, :, pl.ds(pl.multiple_of(layer * piece, 128), piece)]
    out[...] = total * normalizer + n_data[...] * held


def per_device(points, inv_scale, vectors, noise):
    blocks, layers = lax.axis_size("blk"), lax.axis_size("layer")
    chips = blocks // 2
    rows, features = points.shape
    columns = vectors.shape[1]
    piece = rows // layers
    assert blocks == 2 * layers and chips >= 4 and chips & (chips - 1) == 0
    tile = min(256, rows)
    parts = 4
    hbm = pl.BlockSpec(memory_space=pl.ANY)
    dma = pltpu.SemaphoreType.DMA
    peers = chips - 1
    out = pl.pallas_call(
        functools.partial(kernel, chips, layers, parts, tile),
        out_shape=pltpu.VMEM((columns, piece), F32),
        in_specs=[hbm] * 4,
        out_specs=pl.BlockSpec(memory_space=pltpu.VMEM),
        scratch_shapes=[
            pltpu.VMEM((2, rows, features), F32),
            pltpu.VMEM((2, columns, rows), F32),
            pltpu.VMEM((1, features), F32),
            pltpu.VMEM((1, piece), F32),
            pltpu.VMEM((peers, parts, piece // parts, features), F32),
            pltpu.VMEM((2, rows, 4 * features), BF16),
            pltpu.VMEM((2, 2 * columns, rows), BF16),
            pltpu.VMEM((chips, piece, 4 * features), BF16),
            pltpu.VMEM((2, rows, piece), BF16),
            pltpu.VMEM((2, rows, piece), BF16),
            pltpu.VMEM((peers, columns, piece), F32),
            pltpu.VMEM((peers, columns, piece), F32),
            dma((4,)),
            *[dma(()) for _ in range(4)],
            *[dma((peers, parts)) for _ in range(2)],
            *[dma((peers,)) for _ in range(2)],
        ],
        compiler_params=pltpu.CompilerParams(collective_id=0, has_side_effects=True),
    )(points, inv_scale[None, :], vectors.T, noise[None, :])
    return out.T


def solution(mesh):
    placed = (P("blk", None), P(), P("blk", None), P(("blk", "layer")))
    return jax.shard_map(
        per_device, mesh=mesh, in_specs=placed, out_specs=P(("blk", "layer"), None), check_vma=False
    )
```

```python
import functools
import math

import jax
import jax.numpy as jnp
from jax import lax
from jax.experimental import pallas as pl
from jax.experimental.pallas import tpu as pltpu
from jax.sharding import PartitionSpec as P

MESH = pl.DeviceIdType.MESH
LOG2 = math.log(2.0)
UNIT = math.sqrt(5.0) / LOG2
SHIFT = 1.5 / LOG2
REST = 3.0 / LOG2**2 - SHIFT**2
GAIN = LOG2**2 / 3.0 * 2.0**SHIFT
BF16 = jnp.bfloat16
F32 = jnp.float32


def two_terms(value):
    high = value.astype(BF16).astype(F32)
    return high, (value - high).astype(BF16).astype(F32)


def augmented(points, scale, left):
    high, low = two_terms(points * scale)
    held = high + low
    norm = jnp.sum(held * held, axis=1, keepdims=True)
    first = norm.astype(BF16).astype(F32)
    second = (norm - first).astype(BF16).astype(F32)
    third = norm - first - second
    lane = lax.broadcasted_iota(jnp.int32, high.shape, 1)
    at, ones = (0, 3) if left else (3, 0)
    extra = jnp.where(
        lane == at,
        first,
        jnp.where(
            lane == at + 1,
            second,
            jnp.where(
                lane == at + 2,
                third,
                jnp.where((lane >= ones) & (lane < ones + 3), 1.0, 0.0),
            ),
        ),
    )
    if left:
        high, low = -2.0 * high, -2.0 * low
        terms = (high, high, low, extra)
    else:
        terms = (high, low, high, extra)
    return jnp.concatenate([term.astype(BF16) for term in terms], axis=1)


def nt_dot(left, right):
    return lax.dot_general(left, right, (((1,), (1,)), ((), ())), preferred_element_type=F32)


def kernel(
    chips, layers, parts, tile, points, scale, vectors, noise, out,
    p_data, v_data, s_data, n_data, q_in, left, v_left, right, high, low, r_out, r_in, summed,
    own_sem, p_send, p_recv, v_send, v_recv, q_send, q_recv, r_send, r_recv,
):
    block, layer = lax.axis_index("blk"), lax.axis_index("layer")
    core = lax.rem(block, 2)
    chip = block // 2
    rows, columns = p_data.shape[1], v_data.shape[1]
    piece = rows // layers
    mine = pl.ds(pl.multiple_of(layer * piece, piece), piece)
    sibling = (block + 1 - 2 * core, layer)
    others = range(1, chips)
    bits = [1 << d for d in range(chips.bit_length() - 1)]
    part = piece // parts

    def peer(i, same=False):
        return (2 * (chip ^ i) + (core if same else 1 - core), layer)

    barrier = pltpu.get_barrier_semaphore()
    for target in (*(peer(bit, same) for bit in bits for same in (False, True)), sibling):
        pl.semaphore_signal(barrier, inc=1, device_id=target, device_id_type=MESH)

    own = (
        pltpu.make_async_copy(points, p_data.at[0], own_sem.at[0]),
        pltpu.make_async_copy(scale, s_data, own_sem.at[1]),
        pltpu.make_async_copy(vectors, v_data.at[0], own_sem.at[2]),
        pltpu.make_async_copy(noise, n_data, own_sem.at[3]),
    )
    for copy in own:
        copy.start()

    def last_bit(i, h):
        return i & -i if 2 * h >= parts else 1 << (i.bit_length() - 1)

    def nth(i, turn):
        return turn if i * i < chips else (turn + parts // 2) % parts

    def query(i, h):
        bit = last_bit(i, h)
        before = i ^ bit
        at = pl.ds(pl.multiple_of(layer * piece + h * part, part), part)
        return pltpu.make_async_remote_copy(
            q_in.at[before - 1, h] if before else p_data.at[0, at],
            q_in.at[i - 1, h],
            q_send.at[i - 1, h],
            q_recv.at[i - 1, h],
            peer(bit, same=before > 0),
            MESH,
        )

    def relay(i, h):
        for j in others:
            if j ^ last_bit(j, h) == i:
                query(j, h).start()

    def result(i):
        return pltpu.make_async_remote_copy(
            r_out.at[i - 1], r_in.at[i - 1], r_send.at[i - 1], r_recv.at[i - 1], peer(i), MESH
        )

    across = (
        pltpu.make_async_remote_copy(p_data.at[0], p_data.at[1], p_send, p_recv, sibling, MESH),
        pltpu.make_async_remote_copy(v_data.at[0], v_data.at[1], v_send, v_recv, sibling, MESH),
    )

    for copy in own:
        copy.wait()
    unit = s_data[...] * UNIT

    def prepare(slot):
        left[slot] = augmented(p_data[slot], unit, True)
        v_left[slot] = jnp.concatenate(two_terms(v_data[slot]), axis=0).astype(BF16)

    def evaluate(queries, slot, buffer):
        for start in range(0, rows, tile):
            at = pl.ds(start, tile)
            square = jnp.maximum(nt_dot(left[slot, at, :], queries), 1e-20)
            z = -SHIFT - square * lax.rsqrt(square)
            value = (z * z + REST) * jnp.exp2(z)
            high[buffer, at, :] = value.astype(BF16)
            low[buffer, at, :] = (value - value.astype(BF16).astype(F32)).astype(BF16)

    def product(slot, buffer):
        turned = jnp.dot(v_left[slot], high[buffer], preferred_element_type=F32)
        turned_low = jnp.dot(v_left[slot, :columns], low[buffer], preferred_element_type=F32)
        return turned[:columns] + turned[columns:] + turned_low

    def receive(i, h):
        query(i, h).wait_recv()
        relay(i, h)

    def expand(i, h):
        right[i, pl.ds(h * part, part)] = augmented(q_in[i - 1, h], unit, False)

    def answer(i, partial):
        r_out[i - 1] = partial
        result(i).start()

    near, far = 1, chips // 2
    half = piece // 2
    rest = [i for i in others if i not in (near, far)]
    is_last = chip == chips - 1

    def turns(first, last):
        for turn in range(first, last):
            for bit in bits:
                receive(bit, nth(bit, turn))

    def own_second():
        summed[...] += product(1, 3)

    def answer_far(first, second):
        answer(far, jnp.concatenate([second[:, half:], first[:, half:]], axis=1))
        r_out[near - 1] = jnp.concatenate([first[:, :half], second[:, :half]], axis=1)

    pl.semaphore_wait(barrier, 1 + 2 * len(bits))
    for turn in range(parts):
        for bit in bits:
            query(bit, nth(bit, turn)).start()
    for copy in across:
        copy.start()
    prepare(0)
    right[0] = augmented(p_data[0, mine], unit, False)
    evaluate(right[0], 0, 0)
    summed[...] = product(0, 0)
    for copy in across:
        copy.wait()
    prepare(1)

    @pl.when(core == 0)
    def _():
        turns(0, parts // 2)

    evaluate(right[0], 1, 3)

    @pl.when(core == 1)
    def _():
        own_second()
        turns(0, parts // 2)

    for bit in bits:
        for turn in range(parts // 2):
            expand(bit, nth(bit, turn))
    mixed = jnp.concatenate([right[near, :half], right[far, half:]], axis=0)
    evaluate(mixed, 0, 0)
    turns(parts // 2, parts)
    for bit in bits:
        for turn in range(parts // 2, parts):
            expand(bit, nth(bit, turn))
    mixed = jnp.concatenate([right[near, half:], right[far, :half]], axis=0)

    @pl.when(jnp.logical_not(is_last))
    def _():
        evaluate(mixed, 0, 1)
        first = product(0, 0)
        evaluate(right[near], 1, 2)
        answer_far(first, product(0, 1))
        answer(near, r_out[near - 1] + product(1, 2))

    @pl.when(is_last)
    def _():
        evaluate(mixed, 0, 1)
        first = product(0, 0)
        answer_far(first, product(0, 1))

    pl.when(core == 0)(own_second)
    for i in sorted(rest, key=int.bit_count):
        if i not in bits:
            for turn in range(parts):
                receive(i, nth(i, turn))
            for h in range(parts):
                expand(i, h)
        evaluate(right[i], 0, 0)
        evaluate(right[i], 1, 1)
        answer(i, product(0, 0) + product(1, 1))

    @pl.when(is_last)
    def _():
        evaluate(right[near], 1, 2)
        r_out[near - 1] += product(1, 2)
        for i in rest:
            result(i).wait_send()
        result(near).start()

    normalizer = GAIN * float(rows * (2 * layers - 1)) ** (-0.5)
    held = v_data[0, :, pl.ds(pl.multiple_of(layer * piece, 128), piece)]
    gathered = summed[...] * normalizer + n_data[...] * held
    for i in sorted(others, key=lambda i: (i.bit_count(), -i)):
        result(i).wait_recv()
        gathered += r_in[i - 1] * normalizer
    out[...] = gathered
    for i in others:
        for h in range(parts):
            query(i, h).wait_send()

    @pl.when(jnp.logical_not(is_last))
    def _():
        for i in rest:
            result(i).wait_send()

    result(near).wait_send()
    result(far).wait_send()


def per_device(points, inv_scale, vectors, noise):
    blocks, layers = lax.axis_size("blk"), lax.axis_size("layer")
    chips = blocks // 2
    rows, features = points.shape
    columns = vectors.shape[1]
    piece = rows // layers
    assert blocks == 2 * layers and chips >= 4 and chips & (chips - 1) == 0
    tile = min(256, rows)
    parts = 4
    hbm = pl.BlockSpec(memory_space=pl.ANY)
    dma = pltpu.SemaphoreType.DMA
    peers = chips - 1
    out = pl.pallas_call(
        functools.partial(kernel, chips, layers, parts, tile),
        out_shape=pltpu.VMEM((columns, piece), F32),
        in_specs=[hbm] * 4,
        out_specs=pl.BlockSpec(memory_space=pltpu.VMEM),
        scratch_shapes=[
            pltpu.VMEM((2, rows, features), F32),
            pltpu.VMEM((2, columns, rows), F32),
            pltpu.VMEM((1, features), F32),
            pltpu.VMEM((1, piece), F32),
            pltpu.VMEM((peers, parts, piece // parts, features), F32),
            pltpu.VMEM((2, rows, 4 * features), BF16),
            pltpu.VMEM((2, 2 * columns, rows), BF16),
            pltpu.VMEM((chips, piece, 4 * features), BF16),
            pltpu.VMEM((4, rows, piece), BF16),
            pltpu.VMEM((4, rows, piece), BF16),
            pltpu.VMEM((peers, columns, piece), F32),
            pltpu.VMEM((peers, columns, piece), F32),
            pltpu.VMEM((columns, piece), F32),
            dma((4,)),
            *[dma(()) for _ in range(4)],
            *[dma((peers, parts)) for _ in range(2)],
            *[dma((peers,)) for _ in range(2)],
        ],
        compiler_params=pltpu.CompilerParams(collective_id=0, has_side_effects=True),
    )(points, inv_scale[None, :], vectors.T, noise[None, :])
    return out.T


def solution(mesh):
    placed = (P("blk", None), P(), P("blk", None), P(("blk", "layer")))
    return jax.shard_map(
        per_device, mesh=mesh, in_specs=placed, out_specs=P(("blk", "layer"), None), check_vma=False
    )
```
